32 devices in a mesh: band: 4 (over y, core), tile: 8 (over z, x).
Axes of the slice: x: 2, y: 2, z: 4, core: 2. Of those that a mesh axis runs over, the one named last changes fastest.
Arguments:
- patches: bfloat16 [262144, 128], P(('band', 'tile')), may hold values from -6 to 6
- pair_patch: int32 [4096], P(('band', 'tile')), may hold values from 0 to 63
- pair_atm: int32 [4096], P(('band', 'tile')), may hold values from 0 to 4095, as said below
- numerators: int32 [4096, 128, 32], P(('band', 'tile')), may hold values from 0 to 16777215
- counts: int32 [32], P(('band', 'tile')), may hold values from 32 to 128, as said below
Outputs:
- atmosphere: float32 [131072, 128], P(('band', 'tile'))
The draws below stay inside these ranges and needn't reach their ends.
Inputs may be any that keep to these rules, and one draw needn't show every extreme that they name: Block pair_atm[g] is owned by device pair_atm[g] // 128 (band-major device order). Every live pair of device (b, t) targets an owner in band b (any tile) or one of (b - 1, t), (b + 1, t). Among one device's live pairs at most 32 target one owner and at most 16 distinct blocks of one owner; both are reached on some device in every draw. Slots that are not live hold arbitrary blocks in range. `counts`: the value 128 occurs on some device in every draw.
All inputs are finite; a program needn't handle non-finite values.
Results may differ from the reference program's by a relative error of at most 0.0026.
Values sent between devices are 32-bit elements; how exact they have to be, the bound alone decides.
A program may use at most 64 MiB of HBM per device.

```python
import jax
import jax.numpy as jnp
from jax import lax

FLUX = 128
PATCH_BLK = 128
CELL_BLK = 32
PBLK_DEV = 64
CELLS_DEV = 4096
PATCHES = 262144
ALL_PAIRS = 4096
N_BAND = 4
N_TILE = 8


def shuffle_one(subkey):
    return jax.random.permutation(subkey, 2 * PBLK_DEV)


def routing(key):
    base_key = jax.random.fold_in(key, 7)
    subkeys = jax.random.split(base_key, 7)
    devices_all = N_BAND * N_TILE
    pairs_here = 2 * PBLK_DEV
    capacity = PBLK_DEV // 2
    distinct = capacity // 2
    blocks_owned = CELLS_DEV // CELL_BLK
    window = blocks_owned // distinct
    device_ids = jnp.arange(devices_all)
    band_of = (device_ids // N_TILE)[:, None]
    tile_of = (device_ids % N_TILE)[:, None]
    fullest_band = jax.random.randint(subkeys[4], (), 1, N_BAND - 1)
    fullest_tile = jax.random.randint(subkeys[5], (), 0, N_TILE)
    fullest = fullest_band * N_TILE + fullest_tile
    offset_far = jax.random.randint(subkeys[6], (devices_all, 1), 1, N_TILE)
    offset_far = jnp.where(device_ids[:, None] == fullest, N_TILE // 2, offset_far)
    offset_edge = jnp.where(offset_far == N_TILE - 1, 1, offset_far + 1)
    position = jnp.arange(pairs_here)[None, :]
    group = jnp.broadcast_to(position // capacity, (devices_all, pairs_here))
    candidate = jnp.broadcast_to(position % distinct, (devices_all, pairs_here))
    target_band = band_of + jnp.where(group == 1, -1, jnp.where(group == 2, 1, 0))
    target_tile = tile_of + jnp.where(group == 0, offset_far, 0)
    low_edge = (group == 1) & (band_of == 0)
    high_edge = (group == 2) & (band_of == N_BAND - 1)
    at_edge = low_edge | high_edge
    target_band = jnp.where(at_edge, band_of, target_band)
    target_tile = jnp.where(at_edge, tile_of + offset_edge, target_tile) % N_TILE
    owner = target_band * N_TILE + target_tile
    anchor = jax.random.randint(subkeys[0], (devices_all, 4), 0, blocks_owned)
    offsets = jax.random.randint(subkeys[1], (devices_all, 4 * distinct), 0, window)
    anchor_pick = jnp.take_along_axis(anchor, group, axis=1)
    offset_pick = jnp.take_along_axis(offsets, group * distinct + candidate, axis=1)
    local_block = (anchor_pick + candidate * window + offset_pick) % blocks_owned
    global_block = owner * blocks_owned + local_block
    shuffles = jax.vmap(shuffle_one)(jax.random.split(subkeys[2], devices_all))
    global_block = jnp.take_along_axis(global_block, shuffles, axis=1)
    live_counts = jax.random.randint(subkeys[3], (devices_all,), pairs_here // 4, pairs_here + 1)
    live_counts = jnp.where(device_ids == fullest, pairs_here, live_counts)
    return (global_block.reshape(-1).astype(jnp.int32), live_counts.astype(jnp.int32))


def draw_pair_atm(key, part):
    return routing(key)[0]


def draw_counts(key, part):
    return routing(key)[1]


def touch_ends(values, stream_key, least, high):
    extent = values.shape
    index_at = [jax.random.randint(jax.random.fold_in(stream_key, axis), (), 0, extent[axis]) for axis in range(len(extent))]
    values = values.at[tuple(index_at)].set(least)
    longest = extent.index(max(extent))
    index_at[longest] = (index_at[longest] + 1) % extent[longest]
    return values.at[tuple(index_at)].set(high)


def steps_of(stream_key, dims, cuts, smallest, top_value):
    level, own = 1.0, jax.random.fold_in(stream_key, 6)
    for dim, blocks in cuts:
        steps = jnp.exp(jax.random.uniform(jax.random.fold_in(own, dim), (blocks,), jnp.float32, smallest / len(cuts), top_value / len(cuts)))
        level = level * jnp.repeat(steps, dims[dim] // blocks).reshape([-1 if axis == dim else 1 for axis in range(len(dims))])
    return level


def noise(own_key, shape, width, most, shards=(), held_as=jnp.bfloat16):
    loudness = steps_of(own_key, shape, shards, -0.22, 0.18) if shards else 1.0
    result = jax.random.normal(own_key, shape, jnp.float32) * width * loudness
    return jnp.minimum(jnp.maximum(result, -most), most).astype(held_as)


def setup_inputs(seed: int = 0) -> dict:
    key_list = jax.random.split(jax.random.key(seed), 6)
    return {
        "patches": noise(key_list[0], (PATCHES, FLUX), 1.0, 6.0, ((0, 32),)),
        "pair_patch": touch_ends(jax.random.randint(key_list[1], (ALL_PAIRS,), 0, PBLK_DEV), jax.random.fold_in(key_list[1], 1), 0, PBLK_DEV - 1).astype(jnp.int32),
        "pair_atm": draw_pair_atm(jax.random.fold_in(key_list[5], 71), 0),
        "numerators": touch_ends(jax.random.randint(key_list[3], (ALL_PAIRS, PATCH_BLK, CELL_BLK), 0, 16777216), jax.random.fold_in(key_list[3], 1), 0, 16777215).astype(jnp.int32),
        "counts": draw_counts(jax.random.fold_in(key_list[5], 71), 0),
    }


SCALE = 2.0 ** -27


def reference(patches, pair_patch, pair_atm, numerators, counts):
    devices_all = N_BAND * N_TILE
    pairs_here = 2 * PBLK_DEV
    blocks_owned = CELLS_DEV // CELL_BLK
    grouped = patches.reshape(devices_all, PBLK_DEV, PATCH_BLK, FLUX)
    patch_table = pair_patch.reshape(devices_all, pairs_here)
    atm_table = pair_atm.reshape(devices_all, pairs_here)
    numer_table = numerators.reshape(devices_all, pairs_here, PATCH_BLK, CELL_BLK)

    def add_device(accumulated, inputs):
        dev_blocks, patch_index, atm_index, numerator, live_count = inputs
        live_mask = (jnp.arange(pairs_here) < live_count).astype(jnp.float32)
        weight = (numerator.astype(jnp.float32) * SCALE).astype(jnp.bfloat16)
        weight = lax.optimization_barrier(weight).astype(jnp.float32)
        chosen = dev_blocks[patch_index.astype(jnp.int32)].astype(jnp.float32)
        partial_value = jnp.einsum("jpa,jpf->jaf", weight, chosen, precision=lax.Precision.HIGHEST)
        partial_value = partial_value * live_mask[:, None, None]
        return accumulated.at[atm_index.astype(jnp.int32)].add(partial_value), None

    initial = jnp.zeros((devices_all * blocks_owned, CELL_BLK, FLUX), jnp.float32)
    accumulated, unused = lax.scan(add_device, initial, (grouped, patch_table, atm_table, numer_table, counts))
    return accumulated.reshape(devices_all * blocks_owned * CELL_BLK, FLUX)
```

```python
import functools

import jax
import jax.numpy as jnp
from jax import lax
from jax.experimental import pallas as pl
from jax.experimental.pallas import tpu as pltpu
from jax.sharding import PartitionSpec as P

CELLS_DEV = 4096
SCALE = 2.0 ** (-27)
MESH = pl.DeviceIdType.MESH
LANES = 128


def partners(count):
    if count & (count - 1) == 0:
        return [lambda me, k=k: me ^ k for k in range(count - 1, 0, -1)]
    return [lambda me, k=k: lax.rem(me + k, count) for k in range(1, count)]


def pack_kernel(tiles, bucket, blocks_owned, chunk,
                patch_ref, atm_ref, counts_ref, patches_hbm, numer_hbm,
                send_ref, labels_ref,
                patches_v, numer_v, table, used, patch_sem, numer_sems):
    pairs = numer_v.shape[0]
    patch_rows = numer_v.shape[2]
    chunks = pairs // chunk
    buckets = tiles + 2
    patch_copy = pltpu.make_async_copy(patches_hbm, patches_v, patch_sem)
    patch_copy.start()
    copies = []
    for c in range(chunks):
        part = pl.ds(c * chunk, chunk)
        copy = pltpu.make_async_copy(numer_hbm.at[part], numer_v.at[part], numer_sems.at[c])
        copy.start()
        copies.append(copy)
    band = lax.axis_index("band")
    live = counts_ref[0]

    for b in range(buckets):
        used[b] = 0

        @pl.loop(0, blocks_owned, unroll=16)
        def _(i):
            table[b * blocks_owned + i] = -1

        for s in range(bucket):
            labels_ref[b, 0, s] = -1
    patch_copy.wait()
    for c in range(chunks):
        copies[c].wait()

        @pl.when(c * chunk < live)
        def _():
            for j in range(chunk):
                g = c * chunk + j
                is_live = g < live
                atm = atm_ref[g]
                owner = lax.div(atm, blocks_owned)
                block = lax.rem(atm, blocks_owned)
                owner_band = lax.div(owner, tiles)
                owner_tile = lax.rem(owner, tiles)
                b = jnp.where(owner_band == band, owner_tile,
                              jnp.where(owner_band > band, tiles, tiles + 1))
                entry = b * blocks_owned + block
                known = table[entry]
                fresh = known < 0
                new = used[b]
                rank = jnp.where(fresh, new, known)

                @pl.when(is_live)
                def _():
                    table[entry] = rank
                    used[b] = jnp.where(fresh, new + 1, new)
                    labels_ref[b, 0, rank] = block

                slot = jnp.where(is_live, b * bucket + rank, buckets * bucket)
                rows = pl.multiple_of(patch_ref[g] * patch_rows, patch_rows)
                weight = (numer_v[g].astype(jnp.float32) * SCALE).astype(jnp.bfloat16)
                part = jnp.dot(weight, patches_v[pl.ds(rows, patch_rows), :],
                               preferred_element_type=jnp.float32)
                before = send_ref[slot]
                send_ref[slot] = jnp.where(fresh, part, before + part)


def send_kernel(tiles, bands, bucket, send_ref, labels_ref, recv_ref, recv_labels_ref,
                data_send, data_recv, label_send, label_recv):
    band, tile = lax.axis_index("band"), lax.axis_index("tile")
    barrier = pltpu.get_barrier_semaphore()
    steps = partners(tiles)
    for step in steps:
        pl.semaphore_signal(barrier, inc=1, device_id=(band, step(tile)), device_id_type=MESH)

    @pl.when(band < bands - 1)
    def _():
        pl.semaphore_signal(barrier, inc=1, device_id=(band + 1, tile), device_id_type=MESH)

    @pl.when(band > 0)
    def _():
        pl.semaphore_signal(barrier, inc=1, device_id=(band - 1, tile), device_id_type=MESH)

    neighbours = jnp.where(band < bands - 1, 1, 0) + jnp.where(band > 0, 1, 0)
    pl.semaphore_wait(barrier, tiles - 1 + neighbours)

    def pair(source, place, device, sem):
        rows = pl.ds(source * bucket, bucket)
        landing = pl.ds(place * bucket, bucket)
        return (
            pltpu.make_async_remote_copy(
                src_ref=labels_ref.at[source], dst_ref=recv_labels_ref.at[place],
                send_sem=label_send.at[sem], recv_sem=label_recv.at[sem],
                device_id=device, device_id_type=MESH),
            pltpu.make_async_remote_copy(
                src_ref=send_ref.at[rows], dst_ref=recv_ref.at[landing],
                send_sem=data_send.at[sem], recv_sem=data_recv.at[sem],
                device_id=device, device_id_type=MESH),
        )

    inside = [pair(step(tile), tile, (band, step(tile)), k) for k, step in enumerate(steps)]
    upward = pair(tiles, tiles, (band + 1, tile), tiles - 1)
    downward = pair(tiles + 1, tiles + 1, (band - 1, tile), tiles)
    for copies in inside[:2]:
        for copy in copies:
            copy.start()

    @pl.when(band < bands - 1)
    def _():
        for copy in upward:
            copy.start()

    @pl.when(band > 0)
    def _():
        for copy in downward:
            copy.start()

    for copies in inside[2:]:
        for copy in copies:
            copy.start()
    for copies in inside:
        for copy in copies:
            copy.wait()

    @pl.when(band < bands - 1)
    def _():
        for up, down in zip(upward, downward):
            up.wait_send()
            down.wait_recv()

    @pl.when(band > 0)
    def _():
        for up, down in zip(upward, downward):
            down.wait_send()
            up.wait_recv()


def add_kernel(tiles, bands, bucket, labels_ref, recv_labels_ref, send_hbm, recv_hbm, out_ref,
               landed, sems):
    band, tile = lax.axis_index("band"), lax.axis_index("tile")
    buckets = tiles + 2

    def copy_of(b, ref):
        rows = pl.ds(b * bucket, bucket)
        return pltpu.make_async_copy(ref.at[rows], landed.at[rows], sems.at[b])

    for b in range(buckets):
        if b < tiles:
            @pl.when(tile == b)
            def _():
                copy_of(b, send_hbm).start()

            @pl.when(tile != b)
            def _():
                copy_of(b, recv_hbm).start()
        else:
            copy_of(b, recv_hbm).start()
    out_ref[...] = jnp.zeros_like(out_ref)
    for b in range(buckets):
        copy_of(b, recv_hbm).wait()
        if b == tiles:
            valid = band > 0
        elif b == tiles + 1:
            valid = band < bands - 1
        else:
            valid = True
        for s in range(bucket):
            label = recv_labels_ref[b, 0, s]
            if b < tiles:
                label = jnp.where(tile == b, labels_ref[b, 0, s], label)

            @pl.when((label >= 0) & valid)
            def _():
                out_ref[label] += landed[b * bucket + s]


def per_device(tiles, bands, patches, pair_patch, pair_atm, numerators, counts):
    pairs, patch_rows, cell_rows = numerators.shape
    flux = patches.shape[1]
    blocks_owned = CELLS_DEV // cell_rows
    bucket = pairs // 8
    buckets = tiles + 2
    chunk = 16
    smem = pl.BlockSpec(memory_space=pltpu.SMEM)
    vmem = pl.BlockSpec(memory_space=pltpu.VMEM)
    anywhere = pl.BlockSpec(memory_space=pl.ANY)
    labels_shape = jax.ShapeDtypeStruct((buckets, 1, LANES), jnp.int32)
    recv_shape = jax.ShapeDtypeStruct((buckets * bucket, cell_rows, flux), jnp.float32)
    send, labels = pl.pallas_call(
        functools.partial(pack_kernel, tiles, bucket, blocks_owned, chunk),
        out_shape=(jax.ShapeDtypeStruct((buckets * bucket + 1, cell_rows, flux), jnp.float32), labels_shape),
        in_specs=[smem, smem, smem, anywhere, anywhere],
        out_specs=(vmem, smem),
        scratch_shapes=[
            pltpu.VMEM(patches.shape, patches.dtype),
            pltpu.VMEM((pairs, cell_rows, patch_rows), jnp.int32),
            pltpu.SMEM((buckets * blocks_owned,), jnp.int32),
            pltpu.SMEM((buckets,), jnp.int32),
            pltpu.SemaphoreType.DMA,
            pltpu.SemaphoreType.DMA((pairs // chunk,)),
        ],
        name="pack",
    )(pair_patch, pair_atm, counts, patches, jnp.transpose(numerators, (0, 2, 1)))
    recv, recv_labels = pl.pallas_call(
        functools.partial(send_kernel, tiles, bands, bucket),
        out_shape=(recv_shape, labels_shape),
        in_specs=[anywhere, anywhere],
        out_specs=(anywhere, anywhere),
        scratch_shapes=[pltpu.SemaphoreType.DMA((tiles + 1,))] * 4,
        compiler_params=pltpu.CompilerParams(collective_id=0, has_side_effects=True),
        name="exchange",
    )(send, labels)
    out = pl.pallas_call(
        functools.partial(add_kernel, tiles, bands, bucket),
        out_shape=jax.ShapeDtypeStruct((blocks_owned, cell_rows, flux), jnp.float32),
        in_specs=[smem, smem, anywhere, anywhere],
        out_specs=vmem,
        scratch_shapes=[
            pltpu.VMEM(recv_shape.shape, jnp.float32),
            pltpu.SemaphoreType.DMA((buckets,)),
        ],
        name="add",
    )(labels, recv_labels, send, recv)
    return out.reshape(blocks_owned * cell_rows, flux)


def solution(mesh):
    spec = P(("band", "tile"))
    placed = (
        P(("band", "tile"), None),
        spec,
        spec,
        P(("band", "tile"), None, None),
        spec,
    )
    body = functools.partial(per_device, mesh.shape["tile"], mesh.shape["band"])
    return jax.shard_map(body, mesh=mesh, in_specs=placed, out_specs=P(("band", "tile"), None), check_vma=False)
```

```python
import functools

import jax
import jax.numpy as jnp
from jax import lax
from jax.experimental import pallas as pl
from jax.experimental.pallas import tpu as pltpu
from jax.sharding import PartitionSpec as P

CELLS_DEV = 4096
SCALE = 2.0 ** (-27)
MESH = pl.DeviceIdType.MESH
LANES = 128


def partners(count):
    if count & (count - 1) == 0:
        return [lambda me, k=k: me ^ k for k in range(count - 1, 0, -1)]
    return [lambda me, k=k: lax.rem(me + k, count) for k in range(1, count)]


def pack_kernel(tiles, bucket, blocks_owned, chunk,
                patch_ref, atm_ref, counts_ref, patches_hbm, numer_hbm,
                send_ref, labels_ref,
                patches_v, numer_v, table, used, patch_sem, numer_sems):
    pairs = numer_v.shape[0]
    patch_rows = numer_v.shape[2]
    chunks = pairs // chunk
    buckets = tiles + 2
    patch_copy = pltpu.make_async_copy(patches_hbm, patches_v, patch_sem)
    patch_copy.start()
    copies = []
    for c in range(chunks):
        part = pl.ds(c * chunk, chunk)
        copy = pltpu.make_async_copy(numer_hbm.at[part], numer_v.at[part], numer_sems.at[c])
        copy.start()
        copies.append(copy)
    band = lax.axis_index("band")
    live = counts_ref[0]

    for b in range(buckets):
        used[b] = 0

        @pl.loop(0, blocks_owned, unroll=16)
        def _(i):
            table[b * blocks_owned + i] = -1

        for s in range(bucket):
            labels_ref[b, 0, s] = -1
    patch_copy.wait()
    for c in range(chunks):
        copies[c].wait()

        @pl.when(c * chunk < live)
        def _():
            for j in range(chunk):
                g = c * chunk + j
                is_live = g < live
                atm = atm_ref[g]
                owner = lax.div(atm, blocks_owned)
                block = lax.rem(atm, blocks_owned)
                owner_band = lax.div(owner, tiles)
                owner_tile = lax.rem(owner, tiles)
                b = jnp.where(owner_band == band, owner_tile,
                              jnp.where(owner_band > band, tiles, tiles + 1))
                entry = b * blocks_owned + block
                known = table[entry]
                fresh = known < 0
                new = used[b]
                rank = jnp.where(fresh, new, known)

                @pl.when(is_live)
                def _():
                    table[entry] = rank
                    used[b] = jnp.where(fresh, new + 1, new)
                    labels_ref[b, 0, rank] = block

                slot = jnp.where(is_live, b * bucket + rank, buckets * bucket)
                rows = pl.multiple_of(patch_ref[g] * patch_rows, patch_rows)
                weight = (numer_v[g].astype(jnp.float32) * SCALE).astype(jnp.bfloat16)
                part = jnp.dot(weight, patches_v[pl.ds(rows, patch_rows), :],
                               preferred_element_type=jnp.float32)
                before = send_ref[slot]
                send_ref[slot] = jnp.where(fresh, part, before + part)


def send_kernel(tiles, bands, bucket, send_ref, labels_ref, recv_ref, recv_labels_ref,
                data_send, data_recv, label_send, label_recv):
    band, tile = lax.axis_index("band"), lax.axis_index("tile")
    barrier = pltpu.get_barrier_semaphore()
    steps = partners(tiles)
    for step in steps:
        pl.semaphore_signal(barrier, inc=1, device_id=(band, step(tile)), device_id_type=MESH)

    @pl.when(band < bands - 1)
    def _():
        pl.semaphore_signal(barrier, inc=1, device_id=(band + 1, tile), device_id_type=MESH)

    @pl.when(band > 0)
    def _():
        pl.semaphore_signal(barrier, inc=1, device_id=(band - 1, tile), device_id_type=MESH)

    neighbours = jnp.where(band < bands - 1, 1, 0) + jnp.where(band > 0, 1, 0)
    pl.semaphore_wait(barrier, tiles - 1 + neighbours)

    def pair(source, place, device, sem):
        rows = pl.ds(source * bucket, bucket)
        landing = pl.ds(place * bucket, bucket)
        return (
            pltpu.make_async_remote_copy(
                src_ref=labels_ref.at[source], dst_ref=recv_labels_ref.at[place],
                send_sem=label_send.at[sem], recv_sem=label_recv.at[sem],
                device_id=device, device_id_type=MESH),
            pltpu.make_async_remote_copy(
                src_ref=send_ref.at[rows], dst_ref=recv_ref.at[landing],
                send_sem=data_send.at[sem], recv_sem=data_recv.at[sem],
                device_id=device, device_id_type=MESH),
        )

    inside = [pair(step(tile), tile, (band, step(tile)), k) for k, step in enumerate(steps)]
    upward = pair(tiles, tiles, (band + 1, tile), tiles - 1)
    downward = pair(tiles + 1, tiles + 1, (band - 1, tile), tiles)
    for copies in inside[:2]:
        for copy in copies:
            copy.start()

    @pl.when(band < bands - 1)
    def _():
        for copy in upward:
            copy.start()

    @pl.when(band > 0)
    def _():
        for copy in downward:
            copy.start()

    for copies in inside[2:]:
        for copy in copies:
            copy.start()
    for copies in inside:
        for copy in copies:
            copy.wait()

    @pl.when(band < bands - 1)
    def _():
        for up, down in zip(upward, downward):
            up.wait_send()
            down.wait_recv()

    @pl.when(band > 0)
    def _():
        for up, down in zip(upward, downward):
            down.wait_send()
            up.wait_recv()


def add_kernel(tiles, bands, bucket, labels_ref, recv_labels_ref, send_hbm, recv_hbm, out_ref,
               landed, sems):
    band, tile = lax.axis_index("band"), lax.axis_index("tile")
    buckets = tiles + 2

    def copy_of(b, ref):
        rows = pl.ds(b * bucket, bucket)
        return pltpu.make_async_copy(ref.at[rows], landed.at[rows], sems.at[b])

    for b in range(buckets):
        if b < tiles:
            @pl.when(tile == b)
            def _():
                copy_of(b, send_hbm).start()

            @pl.when(tile != b)
            def _():
                copy_of(b, recv_hbm).start()
        else:
            copy_of(b, recv_hbm).start()
    out_ref[...] = jnp.zeros_like(out_ref)
    for b in range(buckets):
        copy_of(b, recv_hbm).wait()
        if b == tiles:
            valid = band > 0
        elif b == tiles + 1:
            valid = band < bands - 1
        else:
            valid = True
        for s in range(bucket):
            label = recv_labels_ref[b, 0, s]
            if b < tiles:
                label = jnp.where(tile == b, labels_ref[b, 0, s], label)

            @pl.when((label >= 0) & valid)
            def _():
                out_ref[label] += landed[b * bucket + s]


def per_device(tiles, bands, patches, pair_patch, pair_atm, numerators, counts):
    pairs, patch_rows, cell_rows = numerators.shape
    flux = patches.shape[1]
    blocks_owned = CELLS_DEV // cell_rows
    bucket = pairs // 8
    buckets = tiles + 2
    chunk = 16
    smem = pl.BlockSpec(memory_space=pltpu.SMEM)
    vmem = pl.BlockSpec(memory_space=pltpu.VMEM)
    anywhere = pl.BlockSpec(memory_space=pl.ANY)
    labels_shape = jax.ShapeDtypeStruct((buckets, 1, LANES), jnp.int32)
    recv_shape = jax.ShapeDtypeStruct((buckets * bucket, cell_rows, flux), jnp.float32)
    send, labels = pl.pallas_call(
        functools.partial(pack_kernel, tiles, bucket, blocks_owned, chunk),
        out_shape=(jax.ShapeDtypeStruct((buckets * bucket + 1, cell_rows, flux), jnp.float32), labels_shape),
        in_specs=[smem, smem, smem, anywhere, anywhere],
        out_specs=(vmem, smem),
        scratch_shapes=[
            pltpu.VMEM(patches.shape, patches.dtype),
            pltpu.VMEM((pairs, cell_rows, patch_rows), jnp.int32),
            pltpu.SMEM((buckets * blocks_owned,), jnp.int32),
            pltpu.SMEM((buckets,), jnp.int32),
            pltpu.SemaphoreType.DMA,
            pltpu.SemaphoreType.DMA((pairs // chunk,)),
        ],
        name="pack",
    )(pair_patch, pair_atm, counts, patches, jnp.transpose(numerators, (0, 2, 1)))
    recv, recv_labels = pl.pallas_call(
        functools.partial(send_kernel, tiles, bands, bucket),
        out_shape=(recv_shape, labels_shape),
        in_specs=[anywhere, anywhere],
        out_specs=(anywhere, anywhere),
        scratch_shapes=[pltpu.SemaphoreType.DMA((tiles + 1,))] * 4,
        compiler_params=pltpu.CompilerParams(collective_id=0, has_side_effects=True),
        name="exchange",
    )(send, labels)
    out = pl.pallas_call(
        functools.partial(add_kernel, tiles, bands, bucket),
        out_shape=jax.ShapeDtypeStruct((blocks_owned, cell_rows, flux), jnp.float32),
        in_specs=[smem, smem, anywhere, anywhere],
        out_specs=vmem,
        scratch_shapes=[
            pltpu.VMEM(recv_shape.shape, jnp.float32),
            pltpu.SemaphoreType.DMA((buckets,)),
        ],
        name="add",
    )(labels, recv_labels, send, recv)
    return out.reshape(blocks_owned * cell_rows, flux)


def ring_order(tiles):
    wide = tiles // 4
    if wide * 4 != tiles or wide % 2:
        return list(range(tiles))
    order = list(range(wide))
    for step, column in enumerate(reversed(range(wide))):
        rows = range(1, 4) if step % 2 == 0 else range(3, 0, -1)
        order += [row * wide + column for row in rows]
    return order


def chosen(values, index):
    picked = values[0]
    for k in range(1, len(values)):
        picked = jnp.where(index == k, values[k], picked)
    return picked


def ring_tile(tiles, tile, steps):
    order = ring_order(tiles)
    position = chosen([order.index(k) for k in range(tiles)], tile)
    return chosen(order, lax.rem(position + steps + tiles, tiles))


def list_kernel(tiles, bands, bucket, blocks_owned, chunk,
                patch_ref, atm_ref, counts_ref, patches_hbm, numer_hbm,
                send_ref, labels_ref,
                patches_v, numer_v, table, used, patch_sem, numer_sems):
    pairs = numer_v.shape[0]
    patch_rows = numer_v.shape[2]
    chunks = pairs // chunk
    patch_copy = pltpu.make_async_copy(patches_hbm, patches_v, patch_sem)
    patch_copy.start()
    copies = []
    for c in range(chunks):
        part = pl.ds(c * chunk, chunk)
        copy = pltpu.make_async_copy(numer_hbm.at[part], numer_v.at[part], numer_sems.at[c])
        copy.start()
        copies.append(copy)
    band, tile = lax.axis_index("band"), lax.axis_index("tile")
    live = counts_ref[0]
    edge = (band == 0) | (band == bands - 1)
    capacity = jnp.where(edge, 2 * bucket, bucket)

    @pl.loop(0, (tiles + 2) * blocks_owned, step=16)
    def _(i):
        for j in range(16):
            table[i + j] = -1

    for b in range(4):
        used[b] = 0
    for s in range(5 * bucket):
        labels_ref[0, s] = -1
    labels_ref[0, LANES - 1] = 0
    patch_copy.wait()
    for c in range(chunks):
        copies[c].wait()

        @pl.when(c * chunk < live)
        def _():
            for j in range(chunk):
                g = c * chunk + j
                is_live = g < live
                atm = atm_ref[g]
                owner = lax.div(atm, blocks_owned)
                block = lax.rem(atm, blocks_owned)
                owner_band = lax.div(owner, tiles)
                owner_tile = lax.rem(owner, tiles)
                inside = owner_band == band
                own = inside & (owner_tile == tile)
                b = jnp.where(inside, owner_tile, jnp.where(owner_band > band, tiles, tiles + 1))
                kind = jnp.where(own, 3, jnp.where(inside, 0, jnp.where(owner_band > band, 1, 2)))
                base = jnp.where(kind == 0, 0, (kind + 1) * bucket)
                entry = b * blocks_owned + block
                known = table[entry]
                fresh = known < 0
                new = used[kind]
                rank = jnp.where(fresh, new, known)
                fits = is_live & ((kind > 0) | (rank < capacity))
                slot = jnp.where(fits, base + rank, 5 * bucket)

                @pl.when(is_live)
                def _():
                    table[entry] = rank
                    used[kind] = jnp.where(fresh, new + 1, new)
                    labels_ref[0, slot] = jnp.where(kind == 0, entry, block)

                @pl.when(is_live & jnp.logical_not(fits))
                def _():
                    labels_ref[0, LANES - 1] = 1

                rows = pl.multiple_of(patch_ref[g] * patch_rows, patch_rows)
                weight = (numer_v[g].astype(jnp.float32) * SCALE).astype(jnp.bfloat16)
                part = jnp.dot(weight, patches_v[pl.ds(rows, patch_rows), :],
                               preferred_element_type=jnp.float32)
                before = send_ref[slot]
                send_ref[slot] = jnp.where(fresh, part, before + part)


def ring_kernel(tiles, bands, bucket, send_ref, labels_ref, recv_ref, beside_ref, table_ref,
                ring_send, ring_recv, beside_send, beside_recv, label_send, label_recv, local_sem):
    band, tile = lax.axis_index("band"), lax.axis_index("tile")
    steps = partners(tiles)
    mine = pltpu.make_async_copy(labels_ref, table_ref.at[band, tile], local_sem)
    mine.start()
    barrier = pltpu.get_barrier_semaphore()
    for step in steps:
        pl.semaphore_signal(barrier, inc=1, device_id=(band, step(tile)), device_id_type=MESH)
    for j in range(1, bands):
        pl.semaphore_signal(barrier, inc=1, device_id=(lax.rem(band + j, bands), tile), device_id_type=MESH)
    pl.semaphore_wait(barrier, tiles + bands - 2)

    reach = tiles // 2
    piece = bucket // 2
    targets = ((band, ring_tile(tiles, tile, 1)), (band, ring_tile(tiles, tile, -1)))

    def hop(way, distance, part):
        rows = pl.ds(part * piece, piece)
        source = send_ref.at[rows] if distance == 1 else recv_ref.at[way, distance - 2, rows]
        return pltpu.make_async_remote_copy(
            src_ref=source, dst_ref=recv_ref.at[way, distance - 1, rows],
            send_sem=ring_send.at[way, distance - 1, part], recv_sem=ring_recv.at[way, distance - 1, part],
            device_id=targets[way], device_id_type=MESH)

    def beside(way, target_band):
        return pltpu.make_async_remote_copy(
            src_ref=send_ref.at[pl.ds((2 + way) * bucket, bucket)], dst_ref=beside_ref.at[way],
            send_sem=beside_send.at[way], recv_sem=beside_recv.at[way],
            device_id=(target_band, tile), device_id_type=MESH)

    def travels(way, distance, part, parts):
        return distance < reach or (part < parts // 2) == (way == 0)

    is_edge = (band == 0) | (band == bands - 1)
    for edge, parts in ((True, 4), (False, 2)):
        @pl.when(is_edge if edge else jnp.logical_not(is_edge))
        def _():
            for part in range(parts):
                for way in range(2):
                    if travels(way, 1, part, parts):
                        hop(way, 1, part).start()

    upward, downward = beside(0, band + 1), beside(1, band - 1)

    @pl.when(band < bands - 1)
    def _():
        upward.start()

    @pl.when(band > 0)
    def _():
        downward.start()

    inside = [
        pltpu.make_async_remote_copy(
            src_ref=labels_ref, dst_ref=table_ref.at[band, tile],
            send_sem=label_send.at[k], recv_sem=label_recv.at[k],
            device_id=(band, step(tile)), device_id_type=MESH)
        for k, step in enumerate(steps)
    ]
    across = [
        pltpu.make_async_remote_copy(
            src_ref=table_ref.at[band], dst_ref=table_ref.at[band],
            send_sem=label_send.at[tiles - 2 + j], recv_sem=label_recv.at[tiles - 2 + j],
            device_id=(lax.rem(band + j, bands), tile), device_id_type=MESH)
        for j in range(1, bands)
    ]
    for copy in inside:
        copy.start()

    for edge, parts in ((True, 4), (False, 2)):
        @pl.when(is_edge if edge else jnp.logical_not(is_edge))
        def _():
            for distance in range(1, reach + 1):
                for part in range(parts):
                    for way in range(2):
                        if not travels(way, distance, part, parts):
                            continue
                        hop(way, distance, part).wait_recv()
                        if distance < reach and travels(way, distance + 1, part, parts):
                            hop(way, distance + 1, part).start()
                if distance == 1:
                    mine.wait()
                    for copy in inside:
                        copy.wait()
                    for copy in across:
                        copy.start()
            for distance in range(1, reach + 1):
                for part in range(parts):
                    for way in range(2):
                        if travels(way, distance, part, parts):
                            hop(way, distance, part).wait_send()
    for copy in across:
        copy.wait()

    @pl.when(band < bands - 1)
    def _():
        upward.wait_send()
        downward.wait_recv()

    @pl.when(band > 0)
    def _():
        downward.wait_send()
        upward.wait_recv()


def take_kernel(tiles, bands, bucket, blocks_owned, labels_ref, table_ref, send_hbm, recv_hbm, beside_hbm, out_ref,
                landed, beside, own, sems):
    band, tile = lax.axis_index("band"), lax.axis_index("tile")
    reach = tiles // 2
    own_copy = pltpu.make_async_copy(send_hbm.at[pl.ds(4 * bucket, bucket)], own, sems.at[2 * reach])
    beside_copy = pltpu.make_async_copy(beside_hbm, beside, sems.at[2 * reach + 1])
    own_copy.start()
    beside_copy.start()
    copies = []
    for distance in range(1, reach + 1):
        for way in range(2):
            copy = pltpu.make_async_copy(recv_hbm.at[way, distance - 1], landed.at[way, distance - 1],
                                         sems.at[2 * (distance - 1) + way])
            copy.start()
            copies.append(copy)
    out_ref[...] = jnp.zeros_like(out_ref)
    own_copy.wait()
    for s in range(bucket):
        label = labels_ref[0, 4 * bucket + s]

        @pl.when(label >= 0)
        def _():
            out_ref[label] += own[s]

    beside_copy.wait()
    for way in range(2):
        other = jnp.clip(band - 1 if way == 0 else band + 1, 0, bands - 1)
        valid = (band > 0) if way == 0 else (band < bands - 1)
        for s in range(bucket):
            label = table_ref[other, tile, 0, (2 + way) * bucket + s]

            @pl.when((label >= 0) & valid)
            def _():
                out_ref[label] += beside[way, s]

    half = jnp.where((band == 0) | (band == bands - 1), bucket, bucket // 2)
    for distance in range(1, reach + 1):
        for way in range(2):
            copies[2 * (distance - 1) + way].wait()
            source = ring_tile(tiles, tile, -distance if way == 0 else distance)
            for s in range(2 * bucket):
                label = table_ref[band, source, 0, s] - tile * blocks_owned
                mine = (label >= 0) & (label < blocks_owned)
                if distance == reach:
                    mine = mine & ((s < half) if way == 0 else (s >= half))

                @pl.when(mine)
                def _():
                    out_ref[label] += landed[way, distance - 1, s]


def adaptive(tiles, bands, patches, pair_patch, pair_atm, numerators, counts):
    pairs, patch_rows, cell_rows = numerators.shape
    flux = patches.shape[1]
    blocks_owned = CELLS_DEV // cell_rows
    bucket = pairs // 8
    reach = tiles // 2
    chunk = 16
    smem = pl.BlockSpec(memory_space=pltpu.SMEM)
    vmem = pl.BlockSpec(memory_space=pltpu.VMEM)
    anywhere = pl.BlockSpec(memory_space=pl.ANY)
    block = (cell_rows, flux)
    recv_shape = jax.ShapeDtypeStruct((2, reach, 2 * bucket) + block, jnp.float32)
    beside_shape = jax.ShapeDtypeStruct((2, bucket) + block, jnp.float32)
    send, labels = pl.pallas_call(
        functools.partial(list_kernel, tiles, bands, bucket, blocks_owned, chunk),
        out_shape=(jax.ShapeDtypeStruct((5 * bucket + 1,) + block, jnp.float32),
                   jax.ShapeDtypeStruct((1, LANES), jnp.int32)),
        in_specs=[smem, smem, smem, anywhere, anywhere],
        out_specs=(vmem, smem),
        scratch_shapes=[
            pltpu.VMEM(patches.shape, patches.dtype),
            pltpu.VMEM((pairs, cell_rows, patch_rows), jnp.int32),
            pltpu.SMEM(((tiles + 2) * blocks_owned,), jnp.int32),
            pltpu.SMEM((4,), jnp.int32),
            pltpu.SemaphoreType.DMA,
            pltpu.SemaphoreType.DMA((pairs // chunk,)),
        ],
        name="list",
    )(pair_patch, pair_atm, counts, patches, jnp.transpose(numerators, (0, 2, 1)))
    recv, beside, table = pl.pallas_call(
        functools.partial(ring_kernel, tiles, bands, bucket),
        out_shape=(recv_shape, beside_shape, jax.ShapeDtypeStruct((bands, tiles, 1, LANES), jnp.int32)),
        in_specs=[anywhere, anywhere],
        out_specs=(anywhere, anywhere, anywhere),
        scratch_shapes=[
            pltpu.SemaphoreType.DMA((2, reach, 4)),
            pltpu.SemaphoreType.DMA((2, reach, 4)),
            pltpu.SemaphoreType.DMA((2,)),
            pltpu.SemaphoreType.DMA((2,)),
            pltpu.SemaphoreType.DMA((tiles + bands - 2,)),
            pltpu.SemaphoreType.DMA((tiles + bands - 2,)),
            pltpu.SemaphoreType.DMA,
        ],
        compiler_params=pltpu.CompilerParams(collective_id=1, has_side_effects=True),
        name="ring",
    )(send, labels)

    def take(patches, pair_patch, pair_atm, numerators, counts, labels, table, send, recv, beside):
        out = pl.pallas_call(
            functools.partial(take_kernel, tiles, bands, bucket, blocks_owned),
            out_shape=jax.ShapeDtypeStruct((blocks_owned,) + block, jnp.float32),
            in_specs=[smem, smem, anywhere, anywhere, anywhere],
            out_specs=vmem,
            scratch_shapes=[
                pltpu.VMEM(recv_shape.shape, jnp.float32),
                pltpu.VMEM(beside_shape.shape, jnp.float32),
                pltpu.VMEM((bucket,) + block, jnp.float32),
                pltpu.SemaphoreType.DMA((2 * reach + 2,)),
            ],
            name="take",
        )(labels, table, send, recv, beside)
        return out.reshape(blocks_owned * cell_rows, flux)

    def padded(patches, pair_patch, pair_atm, numerators, counts, labels, table, send, recv, beside):
        return per_device(tiles, bands, patches, pair_patch, pair_atm, numerators, counts)

    overflowed = jnp.max(table[:, :, 0, LANES - 1]) > 0
    return lax.cond(overflowed, padded, take, patches, pair_patch, pair_atm, numerators, counts,
                    labels, table, send, recv, beside)


def solution(mesh):
    spec = P(("band", "tile"))
    placed = (
        P(("band", "tile"), None),
        spec,
        spec,
        P(("band", "tile"), None, None),
        spec,
    )
    body = functools.partial(adaptive, mesh.shape["tile"], mesh.shape["band"])
    return jax.shard_map(body, mesh=mesh, in_specs=placed, out_specs=P(("band", "tile"), None), check_vma=False)
```

```python
import functools

import jax
import jax.numpy as jnp
from jax import lax
from jax.experimental import pallas as pl
from jax.experimental.pallas import tpu as pltpu
from jax.sharding import PartitionSpec as P

CELLS_DEV = 4096
SCALE = 2.0 ** (-27)
MESH = pl.DeviceIdType.MESH
LANES = 128


def partners(count):
    if count & (count - 1) == 0:
        return [lambda me, k=k: me ^ k for k in range(count - 1, 0, -1)]
    return [lambda me, k=k: lax.rem(me + k, count) for k in range(1, count)]


def pack_kernel(tiles, bucket, blocks_owned, chunk,
                patch_ref, atm_ref, counts_ref, patches_hbm, numer_hbm,
                send_ref, labels_ref,
                patches_v, numer_v, table, used, patch_sem, numer_sems):
    pairs = numer_v.shape[0]
    patch_rows = numer_v.shape[2]
    chunks = pairs // chunk
    buckets = tiles + 2
    patch_copy = pltpu.make_async_copy(patches_hbm, patches_v, patch_sem)
    patch_copy.start()
    copies = []
    for c in range(chunks):
        part = pl.ds(c * chunk, chunk)
        copy = pltpu.make_async_copy(numer_hbm.at[part], numer_v.at[part], numer_sems.at[c])
        copy.start()
        copies.append(copy)
    band = lax.axis_index("band")
    live = counts_ref[0]

    for b in range(buckets):
        used[b] = 0

        @pl.loop(0, blocks_owned, unroll=16)
        def _(i):
            table[b * blocks_owned + i] = -1

        for s in range(bucket):
            labels_ref[b, 0, s] = -1
    patch_copy.wait()
    for c in range(chunks):
        copies[c].wait()

        @pl.when(c * chunk < live)
        def _():
            for j in range(chunk):
                g = c * chunk + j
                is_live = g < live
                atm = atm_ref[g]
                owner = lax.div(atm, blocks_owned)
                block = lax.rem(atm, blocks_owned)
                owner_band = lax.div(owner, tiles)
                owner_tile = lax.rem(owner, tiles)
                b = jnp.where(owner_band == band, owner_tile,
                              jnp.where(owner_band > band, tiles, tiles + 1))
                entry = b * blocks_owned + block
                known = table[entry]
                fresh = known < 0
                new = used[b]
                rank = jnp.where(fresh, new, known)

                @pl.when(is_live)
                def _():
                    table[entry] = rank
                    used[b] = jnp.where(fresh, new + 1, new)
                    labels_ref[b, 0, rank] = block

                slot = jnp.where(is_live, b * bucket + rank, buckets * bucket)
                rows = pl.multiple_of(patch_ref[g] * patch_rows, patch_rows)
                weight = (numer_v[g].astype(jnp.float32) * SCALE).astype(jnp.bfloat16)
                part = jnp.dot(weight, patches_v[pl.ds(rows, patch_rows), :],
                               preferred_element_type=jnp.float32)
                before = send_ref[slot]
                send_ref[slot] = jnp.where(fresh, part, before + part)


def send_kernel(tiles, bands, bucket, send_ref, labels_ref, recv_ref, recv_labels_ref,
                data_send, data_recv, label_send, label_recv):
    band, tile = lax.axis_index("band"), lax.axis_index("tile")
    barrier = pltpu.get_barrier_semaphore()
    steps = partners(tiles)
    for step in steps:
        pl.semaphore_signal(barrier, inc=1, device_id=(band, step(tile)), device_id_type=MESH)

    @pl.when(band < bands - 1)
    def _():
        pl.semaphore_signal(barrier, inc=1, device_id=(band + 1, tile), device_id_type=MESH)

    @pl.when(band > 0)
    def _():
        pl.semaphore_signal(barrier, inc=1, device_id=(band - 1, tile), device_id_type=MESH)

    neighbours = jnp.where(band < bands - 1, 1, 0) + jnp.where(band > 0, 1, 0)
    pl.semaphore_wait(barrier, tiles - 1 + neighbours)

    def pair(source, place, device, sem):
        rows = pl.ds(source * bucket, bucket)
        landing = pl.ds(place * bucket, bucket)
        return (
            pltpu.make_async_remote_copy(
                src_ref=labels_ref.at[source], dst_ref=recv_labels_ref.at[place],
                send_sem=label_send.at[sem], recv_sem=label_recv.at[sem],
                device_id=device, device_id_type=MESH),
            pltpu.make_async_remote_copy(
                src_ref=send_ref.at[rows], dst_ref=recv_ref.at[landing],
                send_sem=data_send.at[sem], recv_sem=data_recv.at[sem],
                device_id=device, device_id_type=MESH),
        )

    inside = [pair(step(tile), tile, (band, step(tile)), k) for k, step in enumerate(steps)]
    upward = pair(tiles, tiles, (band + 1, tile), tiles - 1)
    downward = pair(tiles + 1, tiles + 1, (band - 1, tile), tiles)
    for copies in inside[:2]:
        for copy in copies:
            copy.start()

    @pl.when(band < bands - 1)
    def _():
        for copy in upward:
            copy.start()

    @pl.when(band > 0)
    def _():
        for copy in downward:
            copy.start()

    for copies in inside[2:]:
        for copy in copies:
            copy.start()
    for copies in inside:
        for copy in copies:
            copy.wait()

    @pl.when(band < bands - 1)
    def _():
        for up, down in zip(upward, downward):
            up.wait_send()
            down.wait_recv()

    @pl.when(band > 0)
    def _():
        for up, down in zip(upward, downward):
            down.wait_send()
            up.wait_recv()


def add_kernel(tiles, bands, bucket, labels_ref, recv_labels_ref, send_hbm, recv_hbm, out_ref,
               landed, sems):
    band, tile = lax.axis_index("band"), lax.axis_index("tile")
    buckets = tiles + 2

    def copy_of(b, ref):
        rows = pl.ds(b * bucket, bucket)
        return pltpu.make_async_copy(ref.at[rows], landed.at[rows], sems.at[b])

    for b in range(buckets):
        if b < tiles:
            @pl.when(tile == b)
            def _():
                copy_of(b, send_hbm).start()

            @pl.when(tile != b)
            def _():
                copy_of(b, recv_hbm).start()
        else:
            copy_of(b, recv_hbm).start()
    out_ref[...] = jnp.zeros_like(out_ref)
    for b in range(buckets):
        copy_of(b, recv_hbm).wait()
        if b == tiles:
            valid = band > 0
        elif b == tiles + 1:
            valid = band < bands - 1
        else:
            valid = True
        for s in range(bucket):
            label = recv_labels_ref[b, 0, s]
            if b < tiles:
                label = jnp.where(tile == b, labels_ref[b, 0, s], label)

            @pl.when((label >= 0) & valid)
            def _():
                out_ref[label] += landed[b * bucket + s]


def per_device(tiles, bands, patches, pair_patch, pair_atm, numerators, counts):
    pairs, patch_rows, cell_rows = numerators.shape
    flux = patches.shape[1]
    blocks_owned = CELLS_DEV // cell_rows
    bucket = pairs // 8
    buckets = tiles + 2
    chunk = 16
    smem = pl.BlockSpec(memory_space=pltpu.SMEM)
    vmem = pl.BlockSpec(memory_space=pltpu.VMEM)
    anywhere = pl.BlockSpec(memory_space=pl.ANY)
    labels_shape = jax.ShapeDtypeStruct((buckets, 1, LANES), jnp.int32)
    recv_shape = jax.ShapeDtypeStruct((buckets * bucket, cell_rows, flux), jnp.float32)
    send, labels = pl.pallas_call(
        functools.partial(pack_kernel, tiles, bucket, blocks_owned, chunk),
        out_shape=(jax.ShapeDtypeStruct((buckets * bucket + 1, cell_rows, flux), jnp.float32), labels_shape),
        in_specs=[smem, smem, smem, anywhere, anywhere],
        out_specs=(vmem, smem),
        scratch_shapes=[
            pltpu.VMEM(patches.shape, patches.dtype),
            pltpu.VMEM((pairs, cell_rows, patch_rows), jnp.int32),
            pltpu.SMEM((buckets * blocks_owned,), jnp.int32),
            pltpu.SMEM((buckets,), jnp.int32),
            pltpu.SemaphoreType.DMA,
            pltpu.SemaphoreType.DMA((pairs // chunk,)),
        ],
        name="pack",
    )(pair_patch, pair_atm, counts, patches, jnp.transpose(numerators, (0, 2, 1)))
    recv, recv_labels = pl.pallas_call(
        functools.partial(send_kernel, tiles, bands, bucket),
        out_shape=(recv_shape, labels_shape),
        in_specs=[anywhere, anywhere],
        out_specs=(anywhere, anywhere),
        scratch_shapes=[pltpu.SemaphoreType.DMA((tiles + 1,))] * 4,
        compiler_params=pltpu.CompilerParams(collective_id=0, has_side_effects=True),
        name="exchange",
    )(send, labels)
    out = pl.pallas_call(
        functools.partial(add_kernel, tiles, bands, bucket),
        out_shape=jax.ShapeDtypeStruct((blocks_owned, cell_rows, flux), jnp.float32),
        in_specs=[smem, smem, anywhere, anywhere],
        out_specs=vmem,
        scratch_shapes=[
            pltpu.VMEM(recv_shape.shape, jnp.float32),
            pltpu.SemaphoreType.DMA((buckets,)),
        ],
        name="add",
    )(labels, recv_labels, send, recv)
    return out.reshape(blocks_owned * cell_rows, flux)


def ring_order(tiles):
    wide = tiles // 4
    if wide * 4 != tiles or wide % 2:
        return list(range(tiles))
    order = list(range(wide))
    for step, column in enumerate(reversed(range(wide))):
        rows = range(1, 4) if step % 2 == 0 else range(3, 0, -1)
        order += [row * wide + column for row in rows]
    return order


def chosen(values, index):
    picked = values[0]
    for k in range(1, len(values)):
        picked = jnp.where(index == k, values[k], picked)
    return picked


def ring_tile(tiles, tile, steps):
    order = ring_order(tiles)
    position = chosen([order.index(k) for k in range(tiles)], tile)
    return chosen(order, lax.rem(position + steps + tiles, tiles))


def list_kernel(tiles, bands, bucket, blocks_owned, chunk,
                patch_ref, atm_ref, counts_ref, patches_hbm, numer_hbm,
                send_ref, labels_ref,
                patches_v, numer_v, table, used, slots, firsts, patch_sem, numer_sems):
    pairs = numer_v.shape[0]
    patch_rows = numer_v.shape[2]
    chunks = pairs // chunk
    patch_copy = pltpu.make_async_copy(patches_hbm, patches_v, patch_sem)
    patch_copy.start()
    copies = []
    for c in range(chunks):
        part = pl.ds(c * chunk, chunk)
        copy = pltpu.make_async_copy(numer_hbm.at[part], numer_v.at[part], numer_sems.at[c])
        copy.start()
        copies.append(copy)
    band, tile = lax.axis_index("band"), lax.axis_index("tile")
    live = counts_ref[0]
    edge = (band == 0) | (band == bands - 1)
    capacity = jnp.where(edge, 2 * bucket, bucket)

    @pl.loop(0, (tiles + 2) * blocks_owned, step=16)
    def _(i):
        for j in range(16):
            table[i + j] = -1

    for b in range(4):
        used[b] = 0
    for s in range(5 * bucket):
        labels_ref[0, s] = -1
    labels_ref[0, LANES - 1] = 0

    @pl.loop(0, live)
    def _(g):
        atm = atm_ref[g]
        owner = lax.div(atm, blocks_owned)
        block = lax.rem(atm, blocks_owned)
        owner_band = lax.div(owner, tiles)
        owner_tile = lax.rem(owner, tiles)
        inside = owner_band == band
        own = inside & (owner_tile == tile)
        b = jnp.where(inside, owner_tile, jnp.where(owner_band > band, tiles, tiles + 1))
        kind = jnp.where(own, 3, jnp.where(inside, 0, jnp.where(owner_band > band, 1, 2)))
        base = jnp.where(kind == 0, 0, (kind + 1) * bucket)
        entry = b * blocks_owned + block
        known = table[entry]
        fresh = known < 0
        new = used[kind]
        rank = jnp.where(fresh, new, known)
        fits = (kind > 0) | (rank < capacity)
        slot = jnp.where(fits, base + rank, 5 * bucket)
        table[entry] = rank
        used[kind] = jnp.where(fresh, new + 1, new)
        labels_ref[0, slot] = jnp.where(kind == 0, entry, block)
        labels_ref[0, LANES - 1] = jnp.where(fits, labels_ref[0, LANES - 1], 1)
        slots[g] = slot
        firsts[g] = jnp.where(fresh, 1, 0)

    @pl.loop(live, pairs)
    def _(g):
        slots[g] = 5 * bucket
        firsts[g] = 1

    patch_copy.wait()
    for c in range(chunks):
        copies[c].wait()

        @pl.when(c * chunk < live)
        def _():
            for j in range(chunk):
                g = c * chunk + j
                slot = slots[g]
                rows = pl.multiple_of(patch_ref[g] * patch_rows, patch_rows)
                weight = (numer_v[g].astype(jnp.float32) * SCALE).astype(jnp.bfloat16)
                part = jnp.dot(weight, patches_v[pl.ds(rows, patch_rows), :],
                               preferred_element_type=jnp.float32)
                before = send_ref[slot]
                send_ref[slot] = jnp.where(firsts[g] == 1, part, before + part)


def ring_kernel(tiles, bands, bucket, send_ref, labels_ref, recv_ref, beside_ref, table_ref,
                ring_send, ring_recv, beside_send, beside_recv, label_send, label_recv, local_sem):
    band, tile = lax.axis_index("band"), lax.axis_index("tile")
    steps = partners(tiles)
    mine = pltpu.make_async_copy(labels_ref, table_ref.at[band, tile], local_sem)
    mine.start()
    barrier = pltpu.get_barrier_semaphore()
    for step in steps:
        pl.semaphore_signal(barrier, inc=1, device_id=(band, step(tile)), device_id_type=MESH)
    for j in range(1, bands):
        pl.semaphore_signal(barrier, inc=1, device_id=(lax.rem(band + j, bands), tile), device_id_type=MESH)
    pl.semaphore_wait(barrier, tiles + bands - 2)

    reach = tiles // 2
    piece = bucket // 2
    targets = ((band, ring_tile(tiles, tile, 1)), (band, ring_tile(tiles, tile, -1)))

    def hop(way, distance, part):
        rows = pl.ds(part * piece, piece)
        source = send_ref.at[rows] if distance == 1 else recv_ref.at[way, distance - 2, rows]
        return pltpu.make_async_remote_copy(
            src_ref=source, dst_ref=recv_ref.at[way, distance - 1, rows],
            send_sem=ring_send.at[way, distance - 1, part], recv_sem=ring_recv.at[way, distance - 1, part],
            device_id=targets[way], device_id_type=MESH)

    def beside(way, target_band):
        return pltpu.make_async_remote_copy(
            src_ref=send_ref.at[pl.ds((2 + way) * bucket, bucket)], dst_ref=beside_ref.at[way],
            send_sem=beside_send.at[way], recv_sem=beside_recv.at[way],
            device_id=(target_band, tile), device_id_type=MESH)

    def travels(way, distance, part, parts):
        return distance < reach or (part < parts // 2) == (way == 0)

    is_edge = (band == 0) | (band == bands - 1)
    for edge, parts in ((True, 4), (False, 2)):
        @pl.when(is_edge if edge else jnp.logical_not(is_edge))
        def _():
            for part in range(parts):
                for way in range(2):
                    if travels(way, 1, part, parts):
                        hop(way, 1, part).start()

    upward, downward = beside(0, band + 1), beside(1, band - 1)

    @pl.when(band < bands - 1)
    def _():
        upward.start()

    @pl.when(band > 0)
    def _():
        downward.start()

    inside = [
        pltpu.make_async_remote_copy(
            src_ref=labels_ref, dst_ref=table_ref.at[band, tile],
            send_sem=label_send.at[k], recv_sem=label_recv.at[k],
            device_id=(band, step(tile)), device_id_type=MESH)
        for k, step in enumerate(steps)
    ]
    across = [
        pltpu.make_async_remote_copy(
            src_ref=table_ref.at[band], dst_ref=table_ref.at[band],
            send_sem=label_send.at[tiles - 2 + j], recv_sem=label_recv.at[tiles - 2 + j],
            device_id=(lax.rem(band + j, bands), tile), device_id_type=MESH)
        for j in range(1, bands)
    ]
    for copy in inside:
        copy.start()

    for edge, parts in ((True, 4), (False, 2)):
        @pl.when(is_edge if edge else jnp.logical_not(is_edge))
        def _():
            for distance in range(1, reach + 1):
                for part in range(parts):
                    for way in range(2):
                        if not travels(way, distance, part, parts):
                            continue
                        hop(way, distance, part).wait_recv()
                        if distance < reach and travels(way, distance + 1, part, parts):
                            hop(way, distance + 1, part).start()
                if distance == 1:
                    mine.wait()
                    for copy in inside:
                        copy.wait()
                    for copy in across:
                        copy.start()
            for distance in range(1, reach + 1):
                for part in range(parts):
                    for way in range(2):
                        if travels(way, distance, part, parts):
                            hop(way, distance, part).wait_send()
    for copy in across:
        copy.wait()

    @pl.when(band < bands - 1)
    def _():
        upward.wait_send()
        downward.wait_recv()

    @pl.when(band > 0)
    def _():
        downward.wait_send()
        upward.wait_recv()


def take_kernel(tiles, bands, bucket, blocks_owned, labels_ref, table_ref, send_hbm, recv_hbm, beside_hbm, out_ref,
                landed, beside, own, found_row, found_label, sems):
    band, tile = lax.axis_index("band"), lax.axis_index("tile")
    reach = tiles // 2
    own_copy = pltpu.make_async_copy(send_hbm.at[pl.ds(4 * bucket, bucket)], own, sems.at[0])
    beside_copy = pltpu.make_async_copy(beside_hbm, beside, sems.at[1])
    own_copy.start()
    beside_copy.start()

    half = jnp.where((band == 0) | (band == bands - 1), bucket, bucket // 2)
    found = jnp.int32(0)
    for way in range(2):
        for distance in range(1, reach + 1):
            source = ring_tile(tiles, tile, -distance if way == 0 else distance)
            for s in range(2 * bucket):
                label = table_ref[band, source, 0, s] - tile * blocks_owned
                mine = (label >= 0) & (label < blocks_owned)
                if distance == reach:
                    mine = mine & ((s < half) if way == 0 else (s >= half))
                found_row[found] = (way * reach + distance - 1) * 2 * bucket + s
                found_label[found] = label
                found = found + jnp.where(mine, 1, 0)

    def fetch(i):
        return pltpu.make_async_copy(recv_hbm.at[found_row[i]], landed.at[i], sems.at[2])

    @pl.loop(0, found)
    def _(i):
        fetch(i).start()

    out_ref[...] = jnp.zeros_like(out_ref)
    own_copy.wait()
    for s in range(bucket):
        label = labels_ref[0, 4 * bucket + s]

        @pl.when(label >= 0)
        def _():
            out_ref[label] += own[s]

    beside_copy.wait()
    for way in range(2):
        other = jnp.clip(band - 1 if way == 0 else band + 1, 0, bands - 1)
        valid = (band > 0) if way == 0 else (band < bands - 1)
        for s in range(bucket):
            label = table_ref[other, tile, 0, (2 + way) * bucket + s]

            @pl.when((label >= 0) & valid)
            def _():
                out_ref[label] += beside[way, s]

    @pl.loop(0, found)
    def _(i):
        fetch(i).wait()

    @pl.loop(0, found)
    def _(i):
        out_ref[found_label[i]] += landed[i]


def adaptive(tiles, bands, patches, pair_patch, pair_atm, numerators, counts):
    pairs, patch_rows, cell_rows = numerators.shape
    flux = patches.shape[1]
    blocks_owned = CELLS_DEV // cell_rows
    bucket = pairs // 8
    reach = tiles // 2
    chunk = 16
    smem = pl.BlockSpec(memory_space=pltpu.SMEM)
    vmem = pl.BlockSpec(memory_space=pltpu.VMEM)
    anywhere = pl.BlockSpec(memory_space=pl.ANY)
    block = (cell_rows, flux)
    recv_shape = jax.ShapeDtypeStruct((2, reach, 2 * bucket) + block, jnp.float32)
    beside_shape = jax.ShapeDtypeStruct((2, bucket) + block, jnp.float32)
    send, labels = pl.pallas_call(
        functools.partial(list_kernel, tiles, bands, bucket, blocks_owned, chunk),
        out_shape=(jax.ShapeDtypeStruct((5 * bucket + 1,) + block, jnp.float32),
                   jax.ShapeDtypeStruct((1, LANES), jnp.int32)),
        in_specs=[smem, smem, smem, anywhere, anywhere],
        out_specs=(vmem, smem),
        scratch_shapes=[
            pltpu.VMEM(patches.shape, patches.dtype),
            pltpu.VMEM((pairs, cell_rows, patch_rows), jnp.int32),
            pltpu.SMEM(((tiles + 2) * blocks_owned,), jnp.int32),
            pltpu.SMEM((4,), jnp.int32),
            pltpu.SMEM((pairs,), jnp.int32),
            pltpu.SMEM((pairs,), jnp.int32),
            pltpu.SemaphoreType.DMA,
            pltpu.SemaphoreType.DMA((pairs // chunk,)),
        ],
        name="list",
    )(pair_patch, pair_atm, counts, patches, jnp.transpose(numerators, (0, 2, 1)))
    recv, beside, table = pl.pallas_call(
        functools.partial(ring_kernel, tiles, bands, bucket),
        out_shape=(recv_shape, beside_shape, jax.ShapeDtypeStruct((bands, tiles, 1, LANES), jnp.int32)),
        in_specs=[anywhere, anywhere],
        out_specs=(anywhere, anywhere, anywhere),
        scratch_shapes=[
            pltpu.SemaphoreType.DMA((2, reach, 4)),
            pltpu.SemaphoreType.DMA((2, reach, 4)),
            pltpu.SemaphoreType.DMA((2,)),
            pltpu.SemaphoreType.DMA((2,)),
            pltpu.SemaphoreType.DMA((tiles + bands - 2,)),
            pltpu.SemaphoreType.DMA((tiles + bands - 2,)),
            pltpu.SemaphoreType.DMA,
        ],
        compiler_params=pltpu.CompilerParams(collective_id=1, has_side_effects=True),
        name="ring",
    )(send, labels)

    def take(patches, pair_patch, pair_atm, numerators, counts, labels, table, send, recv, beside):
        out = pl.pallas_call(
            functools.partial(take_kernel, tiles, bands, bucket, blocks_owned),
            out_shape=jax.ShapeDtypeStruct((blocks_owned,) + block, jnp.float32),
            in_specs=[smem, smem, anywhere, anywhere, anywhere],
            out_specs=vmem,
            scratch_shapes=[
                pltpu.VMEM((4 * reach * bucket,) + block, jnp.float32),
                pltpu.VMEM(beside_shape.shape, jnp.float32),
                pltpu.VMEM((bucket,) + block, jnp.float32),
                pltpu.SMEM((4 * reach * bucket + 1,), jnp.int32),
                pltpu.SMEM((4 * reach * bucket + 1,), jnp.int32),
                pltpu.SemaphoreType.DMA((3,)),
            ],
            name="take",
        )(labels, table, send, recv.reshape((4 * reach * bucket,) + block), beside)
        return out.reshape(blocks_owned * cell_rows, flux)

    def padded(patches, pair_patch, pair_atm, numerators, counts, labels, table, send, recv, beside):
        return per_device(tiles, bands, patches, pair_patch, pair_atm, numerators, counts)

    overflowed = jnp.max(table[:, :, 0, LANES - 1]) > 0
    return lax.cond(overflowed, padded, take, patches, pair_patch, pair_atm, numerators, counts,
                    labels, table, send, recv, beside)


def solution(mesh):
    spec = P(("band", "tile"))
    placed = (
        P(("band", "tile"), None),
        spec,
        spec,
        P(("band", "tile"), None, None),
        spec,
    )
    body = functools.partial(adaptive, mesh.shape["tile"], mesh.shape["band"])
    return jax.shard_map(body, mesh=mesh, in_specs=placed, out_specs=P(("band", "tile"), None), check_vma=False)
```

```python
import functools

import jax
import jax.numpy as jnp
from jax import lax
from jax.experimental import pallas as pl
from jax.experimental.pallas import tpu as pltpu
from jax.sharding import PartitionSpec as P

CELLS_DEV = 4096
SCALE = 2.0 ** (-27)
MESH = pl.DeviceIdType.MESH
LANES = 128


def partners(count):
    if count & (count - 1) == 0:
        return [lambda me, k=k: me ^ k for k in range(count - 1, 0, -1)]
    return [lambda me, k=k: lax.rem(me + k, count) for k in range(1, count)]


def pack_kernel(tiles, bucket, blocks_owned, chunk,
                patch_ref, atm_ref, counts_ref, patches_hbm, numer_hbm,
                send_ref, labels_ref,
                patches_v, numer_v, table, used, patch_sem, numer_sems):
    pairs = numer_v.shape[0]
    patch_rows = numer_v.shape[2]
    chunks = pairs // chunk
    buckets = tiles + 2
    patch_copy = pltpu.make_async_copy(patches_hbm, patches_v, patch_sem)
    patch_copy.start()
    copies = []
    for c in range(chunks):
        part = pl.ds(c * chunk, chunk)
        copy = pltpu.make_async_copy(numer_hbm.at[part], numer_v.at[part], numer_sems.at[c])
        copy.start()
        copies.append(copy)
    band = lax.axis_index("band")
    live = counts_ref[0]

    for b in range(buckets):
        used[b] = 0

        @pl.loop(0, blocks_owned, unroll=16)
        def _(i):
            table[b * blocks_owned + i] = -1

        for s in range(bucket):
            labels_ref[b, 0, s] = -1
    patch_copy.wait()
    for c in range(chunks):
        copies[c].wait()

        @pl.when(c * chunk < live)
        def _():
            for j in range(chunk):
                g = c * chunk + j
                is_live = g < live
                atm = atm_ref[g]
                owner = lax.div(atm, blocks_owned)
                block = lax.rem(atm, blocks_owned)
                owner_band = lax.div(owner, tiles)
                owner_tile = lax.rem(owner, tiles)
                b = jnp.where(owner_band == band, owner_tile,
                              jnp.where(owner_band > band, tiles, tiles + 1))
                entry = b * blocks_owned + block
                known = table[entry]
                fresh = known < 0
                new = used[b]
                rank = jnp.where(fresh, new, known)

                @pl.when(is_live)
                def _():
                    table[entry] = rank
                    used[b] = jnp.where(fresh, new + 1, new)
                    labels_ref[b, 0, rank] = block

                slot = jnp.where(is_live, b * bucket + rank, buckets * bucket)
                rows = pl.multiple_of(patch_ref[g] * patch_rows, patch_rows)
                weight = (numer_v[g].astype(jnp.float32) * SCALE).astype(jnp.bfloat16)
                part = jnp.dot(weight, patches_v[pl.ds(rows, patch_rows), :],
                               preferred_element_type=jnp.float32)
                before = send_ref[slot]
                send_ref[slot] = jnp.where(fresh, part, before + part)


def send_kernel(tiles, bands, bucket, send_ref, labels_ref, recv_ref, recv_labels_ref,
                data_send, data_recv, label_send, label_recv):
    band, tile = lax.axis_index("band"), lax.axis_index("tile")
    barrier = pltpu.get_barrier_semaphore()
    steps = partners(tiles)
    for step in steps:
        pl.semaphore_signal(barrier, inc=1, device_id=(band, step(tile)), device_id_type=MESH)

    @pl.when(band < bands - 1)
    def _():
        pl.semaphore_signal(barrier, inc=1, device_id=(band + 1, tile), device_id_type=MESH)

    @pl.when(band > 0)
    def _():
        pl.semaphore_signal(barrier, inc=1, device_id=(band - 1, tile), device_id_type=MESH)

    neighbours = jnp.where(band < bands - 1, 1, 0) + jnp.where(band > 0, 1, 0)
    pl.semaphore_wait(barrier, tiles - 1 + neighbours)

    def pair(source, place, device, sem):
        rows = pl.ds(source * bucket, bucket)
        landing = pl.ds(place * bucket, bucket)
        return (
            pltpu.make_async_remote_copy(
                src_ref=labels_ref.at[source], dst_ref=recv_labels_ref.at[place],
                send_sem=label_send.at[sem], recv_sem=label_recv.at[sem],
                device_id=device, device_id_type=MESH),
            pltpu.make_async_remote_copy(
                src_ref=send_ref.at[rows], dst_ref=recv_ref.at[landing],
                send_sem=data_send.at[sem], recv_sem=data_recv.at[sem],
                device_id=device, device_id_type=MESH),
        )

    inside = [pair(step(tile), tile, (band, step(tile)), k) for k, step in enumerate(steps)]
    upward = pair(tiles, tiles, (band + 1, tile), tiles - 1)
    downward = pair(tiles + 1, tiles + 1, (band - 1, tile), tiles)
    for copies in inside[:2]:
        for copy in copies:
            copy.start()

    @pl.when(band < bands - 1)
    def _():
        for copy in upward:
            copy.start()

    @pl.when(band > 0)
    def _():
        for copy in downward:
            copy.start()

    for copies in inside[2:]:
        for copy in copies:
            copy.start()
    for copies in inside:
        for copy in copies:
            copy.wait()

    @pl.when(band < bands - 1)
    def _():
        for up, down in zip(upward, downward):
            up.wait_send()
            down.wait_recv()

    @pl.when(band > 0)
    def _():
        for up, down in zip(upward, downward):
            down.wait_send()
            up.wait_recv()


def add_kernel(tiles, bands, bucket, labels_ref, recv_labels_ref, send_hbm, recv_hbm, out_ref,
               landed, sems):
    band, tile = lax.axis_index("band"), lax.axis_index("tile")
    buckets = tiles + 2

    def copy_of(b, ref):
        rows = pl.ds(b * bucket, bucket)
        return pltpu.make_async_copy(ref.at[rows], landed.at[rows], sems.at[b])

    for b in range(buckets):
        if b < tiles:
            @pl.when(tile == b)
            def _():
                copy_of(b, send_hbm).start()

            @pl.when(tile != b)
            def _():
                copy_of(b, recv_hbm).start()
        else:
            copy_of(b, recv_hbm).start()
    out_ref[...] = jnp.zeros_like(out_ref)
    for b in range(buckets):
        copy_of(b, recv_hbm).wait()
        if b == tiles:
            valid = band > 0
        elif b == tiles + 1:
            valid = band < bands - 1
        else:
            valid = True
        for s in range(bucket):
            label = recv_labels_ref[b, 0, s]
            if b < tiles:
                label = jnp.where(tile == b, labels_ref[b, 0, s], label)

            @pl.when((label >= 0) & valid)
            def _():
                out_ref[label] += landed[b * bucket + s]


def per_device(tiles, bands, patches, pair_patch, pair_atm, numerators, counts):
    pairs, patch_rows, cell_rows = numerators.shape
    flux = patches.shape[1]
    blocks_owned = CELLS_DEV // cell_rows
    bucket = pairs // 8
    buckets = tiles + 2
    chunk = 16
    smem = pl.BlockSpec(memory_space=pltpu.SMEM)
    vmem = pl.BlockSpec(memory_space=pltpu.VMEM)
    anywhere = pl.BlockSpec(memory_space=pl.ANY)
    labels_shape = jax.ShapeDtypeStruct((buckets, 1, LANES), jnp.int32)
    recv_shape = jax.ShapeDtypeStruct((buckets * bucket, cell_rows, flux), jnp.float32)
    send, labels = pl.pallas_call(
        functools.partial(pack_kernel, tiles, bucket, blocks_owned, chunk),
        out_shape=(jax.ShapeDtypeStruct((buckets * bucket + 1, cell_rows, flux), jnp.float32), labels_shape),
        in_specs=[smem, smem, smem, anywhere, anywhere],
        out_specs=(vmem, smem),
        scratch_shapes=[
            pltpu.VMEM(patches.shape, patches.dtype),
            pltpu.VMEM((pairs, cell_rows, patch_rows), jnp.int32),
            pltpu.SMEM((buckets * blocks_owned,), jnp.int32),
            pltpu.SMEM((buckets,), jnp.int32),
            pltpu.SemaphoreType.DMA,
            pltpu.SemaphoreType.DMA((pairs // chunk,)),
        ],
        name="pack",
    )(pair_patch, pair_atm, counts, patches, jnp.transpose(numerators, (0, 2, 1)))
    recv, recv_labels = pl.pallas_call(
        functools.partial(send_kernel, tiles, bands, bucket),
        out_shape=(recv_shape, labels_shape),
        in_specs=[anywhere, anywhere],
        out_specs=(anywhere, anywhere),
        scratch_shapes=[pltpu.SemaphoreType.DMA((tiles + 1,))] * 4,
        compiler_params=pltpu.CompilerParams(collective_id=0, has_side_effects=True),
        name="exchange",
    )(send, labels)
    out = pl.pallas_call(
        functools.partial(add_kernel, tiles, bands, bucket),
        out_shape=jax.ShapeDtypeStruct((blocks_owned, cell_rows, flux), jnp.float32),
        in_specs=[smem, smem, anywhere, anywhere],
        out_specs=vmem,
        scratch_shapes=[
            pltpu.VMEM(recv_shape.shape, jnp.float32),
            pltpu.SemaphoreType.DMA((buckets,)),
        ],
        name="add",
    )(labels, recv_labels, send, recv)
    return out.reshape(blocks_owned * cell_rows, flux)


def ring_order(tiles):
    wide = tiles // 4
    if wide * 4 != tiles or wide % 2:
        return list(range(tiles))
    order = list(range(wide))
    for step, column in enumerate(reversed(range(wide))):
        rows = range(1, 4) if step % 2 == 0 else range(3, 0, -1)
        order += [row * wide + column for row in rows]
    return order


def chosen(values, index):
    picked = values[0]
    for k in range(1, len(values)):
        picked = jnp.where(index == k, values[k], picked)
    return picked


def ring_tile(tiles, tile, steps):
    order = ring_order(tiles)
    position = chosen([order.index(k) for k in range(tiles)], tile)
    return chosen(order, lax.rem(position + steps + tiles, tiles))


def list_kernel(tiles, bands, bucket, blocks_owned, chunk,
                patch_ref, atm_ref, counts_ref, patches_hbm, numer_hbm,
                send_ref, labels_ref,
                patches_v, numer_v, table, used, patch_sem, numer_sems):
    pairs = numer_v.shape[0]
    patch_rows = numer_v.shape[2]
    chunks = pairs // chunk
    patch_copy = pltpu.make_async_copy(patches_hbm, patches_v, patch_sem)
    patch_copy.start()
    copies = []
    for c in range(chunks):
        part = pl.ds(c * chunk, chunk)
        copy = pltpu.make_async_copy(numer_hbm.at[part], numer_v.at[part], numer_sems.at[c])
        copy.start()
        copies.append(copy)
    band, tile = lax.axis_index("band"), lax.axis_index("tile")
    live = counts_ref[0]
    edge = (band == 0) | (band == bands - 1)
    capacity = jnp.where(edge, 2 * bucket, bucket)

    @pl.loop(0, (tiles + 2) * blocks_owned, step=16)
    def _(i):
        for j in range(16):
            table[i + j] = -1

    for b in range(4):
        used[b] = 0
    for s in range(5 * bucket):
        labels_ref[0, s] = -1
    labels_ref[0, LANES - 1] = 0
    patch_copy.wait()
    for c in range(chunks):
        copies[c].wait()

        @pl.when(c * chunk < live)
        def _():
            for j in range(chunk):
                g = c * chunk + j
                is_live = g < live
                atm = atm_ref[g]
                owner = lax.div(atm, blocks_owned)
                block = lax.rem(atm, blocks_owned)
                owner_band = lax.div(owner, tiles)
                owner_tile = lax.rem(owner, tiles)
                inside = owner_band == band
                own = inside & (owner_tile == tile)
                b = jnp.where(inside, owner_tile, jnp.where(owner_band > band, tiles, tiles + 1))
                kind = jnp.where(own, 3, jnp.where(inside, 0, jnp.where(owner_band > band, 1, 2)))
                base = jnp.where(kind == 0, 0, (kind + 1) * bucket)
                entry = b * blocks_owned + block
                known = table[entry]
                fresh = known < 0
                new = used[kind]
                rank = jnp.where(fresh, new, known)
                fits = is_live & ((kind > 0) | (rank < capacity))
                slot = jnp.where(fits, base + rank, 5 * bucket)

                @pl.when(is_live)
                def _():
                    table[entry] = rank
                    used[kind] = jnp.where(fresh, new + 1, new)
                    labels_ref[0, slot] = jnp.where(kind == 0, entry, block)

                @pl.when(is_live & jnp.logical_not(fits))
                def _():
                    labels_ref[0, LANES - 1] = 1

                rows = pl.multiple_of(patch_ref[g] * patch_rows, patch_rows)
                weight = (numer_v[g].astype(jnp.float32) * SCALE).astype(jnp.bfloat16)
                part = jnp.dot(weight, patches_v[pl.ds(rows, patch_rows), :],
                               preferred_element_type=jnp.float32)
                before = send_ref[slot]
                send_ref[slot] = jnp.where(fresh, part, before + part)


def ring_kernel(tiles, bands, bucket, send_ref, labels_ref, recv_ref, beside_ref, table_ref,
                ring_send, ring_recv, beside_send, beside_recv, label_send, label_recv, local_sem):
    band, tile = lax.axis_index("band"), lax.axis_index("tile")
    steps = partners(tiles)
    mine = pltpu.make_async_copy(labels_ref, table_ref.at[band, tile], local_sem)
    mine.start()
    barrier = pltpu.get_barrier_semaphore()
    for step in steps:
        pl.semaphore_signal(barrier, inc=1, device_id=(band, step(tile)), device_id_type=MESH)
    for j in range(1, bands):
        pl.semaphore_signal(barrier, inc=1, device_id=(lax.rem(band + j, bands), tile), device_id_type=MESH)
    pl.semaphore_wait(barrier, tiles + bands - 2)

    reach = tiles // 2
    piece = bucket // 2
    targets = ((band, ring_tile(tiles, tile, 1)), (band, ring_tile(tiles, tile, -1)))

    def hop(way, distance, part):
        rows = pl.ds(part * piece, piece)
        source = send_ref.at[rows] if distance == 1 else recv_ref.at[way, distance - 2, rows]
        return pltpu.make_async_remote_copy(
            src_ref=source, dst_ref=recv_ref.at[way, distance - 1, rows],
            send_sem=ring_send.at[way, distance - 1, part], recv_sem=ring_recv.at[way, distance - 1, part],
            device_id=targets[way], device_id_type=MESH)

    def beside(way, target_band):
        return pltpu.make_async_remote_copy(
            src_ref=send_ref.at[pl.ds((2 + way) * bucket, bucket)], dst_ref=beside_ref.at[way],
            send_sem=beside_send.at[way], recv_sem=beside_recv.at[way],
            device_id=(target_band, tile), device_id_type=MESH)

    def travels(way, distance, part, parts):
        return distance < reach or (part < parts // 2) == (way == 0)

    is_edge = (band == 0) | (band == bands - 1)
    for edge, parts in ((True, 4), (False, 2)):
        @pl.when(is_edge if edge else jnp.logical_not(is_edge))
        def _():
            for part in range(parts):
                for way in range(2):
                    if travels(way, 1, part, parts):
                        hop(way, 1, part).start()

    upward, downward = beside(0, band + 1), beside(1, band - 1)

    @pl.when(band < bands - 1)
    def _():
        upward.start()

    @pl.when(band > 0)
    def _():
        downward.start()

    inside = [
        pltpu.make_async_remote_copy(
            src_ref=labels_ref, dst_ref=table_ref.at[band, tile],
            send_sem=label_send.at[k], recv_sem=label_recv.at[k],
            device_id=(band, step(tile)), device_id_type=MESH)
        for k, step in enumerate(steps)
    ]
    across = [
        pltpu.make_async_remote_copy(
            src_ref=table_ref.at[band], dst_ref=table_ref.at[band],
            send_sem=label_send.at[tiles - 2 + j], recv_sem=label_recv.at[tiles - 2 + j],
            device_id=(lax.rem(band + j, bands), tile), device_id_type=MESH)
        for j in range(1, bands)
    ]
    for copy in inside:
        copy.start()

    for edge, parts in ((True, 4), (False, 2)):
        @pl.when(is_edge if edge else jnp.logical_not(is_edge))
        def _():
            for distance in range(1, reach + 1):
                for part in range(parts):
                    for way in range(2):
                        if not travels(way, distance, part, parts):
                            continue
                        hop(way, distance, part).wait_recv()
                        if distance < reach and travels(way, distance + 1, part, parts):
                            hop(way, distance + 1, part).start()
                if distance == 1:
                    mine.wait()
                    for copy in inside:
                        copy.wait()
                    for copy in across:
                        copy.start()
            for distance in range(1, reach + 1):
                for part in range(parts):
                    for way in range(2):
                        if travels(way, distance, part, parts):
                            hop(way, distance, part).wait_send()
    for copy in across:
        copy.wait()

    @pl.when(band < bands - 1)
    def _():
        upward.wait_send()
        downward.wait_recv()

    @pl.when(band > 0)
    def _():
        downward.wait_send()
        upward.wait_recv()


def take_kernel(tiles, bands, bucket, blocks_owned, labels_ref, table_ref, send_hbm, recv_hbm, beside_hbm, out_ref,
                landed, beside, own, found_row, found_label, sems):
    band, tile = lax.axis_index("band"), lax.axis_index("tile")
    reach = tiles // 2
    own_copy = pltpu.make_async_copy(send_hbm.at[pl.ds(4 * bucket, bucket)], own, sems.at[0])
    beside_copy = pltpu.make_async_copy(beside_hbm, beside, sems.at[1])
    own_copy.start()
    beside_copy.start()

    half = jnp.where((band == 0) | (band == bands - 1), bucket, bucket // 2)
    found = jnp.int32(0)
    for way in range(2):
        for distance in range(1, reach + 1):
            source = ring_tile(tiles, tile, -distance if way == 0 else distance)
            for s in range(2 * bucket):
                label = table_ref[band, source, 0, s] - tile * blocks_owned
                mine = (label >= 0) & (label < blocks_owned)
                if distance == reach:
                    mine = mine & ((s < half) if way == 0 else (s >= half))
                found_row[found] = (way * reach + distance - 1) * 2 * bucket + s
                found_label[found] = label
                found = found + jnp.where(mine, 1, 0)

    def fetch(i):
        return pltpu.make_async_copy(recv_hbm.at[found_row[i]], landed.at[i], sems.at[2])

    @pl.loop(0, found)
    def _(i):
        fetch(i).start()

    out_ref[...] = jnp.zeros_like(out_ref)
    own_copy.wait()
    for s in range(bucket):
        label = labels_ref[0, 4 * bucket + s]

        @pl.when(label >= 0)
        def _():
            out_ref[label] += own[s]

    beside_copy.wait()
    for way in range(2):
        other = jnp.clip(band - 1 if way == 0 else band + 1, 0, bands - 1)
        valid = (band > 0) if way == 0 else (band < bands - 1)
        for s in range(bucket):
            label = table_ref[other, tile, 0, (2 + way) * bucket + s]

            @pl.when((label >= 0) & valid)
            def _():
                out_ref[label] += beside[way, s]

    @pl.loop(0, found)
    def _(i):
        fetch(i).wait()

    @pl.loop(0, found)
    def _(i):
        out_ref[found_label[i]] += landed[i]


def adaptive(tiles, bands, patches, pair_patch, pair_atm, numerators, counts):
    pairs, patch_rows, cell_rows = numerators.shape
    flux = patches.shape[1]
    blocks_owned = CELLS_DEV // cell_rows
    bucket = pairs // 8
    reach = tiles // 2
    chunk = 16
    smem = pl.BlockSpec(memory_space=pltpu.SMEM)
    vmem = pl.BlockSpec(memory_space=pltpu.VMEM)
    anywhere = pl.BlockSpec(memory_space=pl.ANY)
    block = (cell_rows, flux)
    recv_shape = jax.ShapeDtypeStruct((2, reach, 2 * bucket) + block, jnp.float32)
    beside_shape = jax.ShapeDtypeStruct((2, bucket) + block, jnp.float32)
    send, labels = pl.pallas_call(
        functools.partial(list_kernel, tiles, bands, bucket, blocks_owned, chunk),
        out_shape=(jax.ShapeDtypeStruct((5 * bucket + 1,) + block, jnp.float32),
                   jax.ShapeDtypeStruct((1, LANES), jnp.int32)),
        in_specs=[smem, smem, smem, anywhere, anywhere],
        out_specs=(vmem, smem),
        scratch_shapes=[
            pltpu.VMEM(patches.shape, patches.dtype),
            pltpu.VMEM((pairs, cell_rows, patch_rows), jnp.int32),
            pltpu.SMEM(((tiles + 2) * blocks_owned,), jnp.int32),
            pltpu.SMEM((4,), jnp.int32),
            pltpu.SemaphoreType.DMA,
            pltpu.SemaphoreType.DMA((pairs // chunk,)),
        ],
        name="list",
    )(pair_patch, pair_atm, counts, patches, jnp.transpose(numerators, (0, 2, 1)))
    recv, beside, table = pl.pallas_call(
        functools.partial(ring_kernel, tiles, bands, bucket),
        out_shape=(recv_shape, beside_shape, jax.ShapeDtypeStruct((bands, tiles, 1, LANES), jnp.int32)),
        in_specs=[anywhere, anywhere],
        out_specs=(anywhere, anywhere, anywhere),
        scratch_shapes=[
            pltpu.SemaphoreType.DMA((2, reach, 4)),
            pltpu.SemaphoreType.DMA((2, reach, 4)),
            pltpu.SemaphoreType.DMA((2,)),
            pltpu.SemaphoreType.DMA((2,)),
            pltpu.SemaphoreType.DMA((tiles + bands - 2,)),
            pltpu.SemaphoreType.DMA((tiles + bands - 2,)),
            pltpu.SemaphoreType.DMA,
        ],
        compiler_params=pltpu.CompilerParams(collective_id=1, has_side_effects=True),
        name="ring",
    )(send, labels)

    def take(patches, pair_patch, pair_atm, numerators, counts, labels, table, send, recv, beside):
        out = pl.pallas_call(
            functools.partial(take_kernel, tiles, bands, bucket, blocks_owned),
            out_shape=jax.ShapeDtypeStruct((blocks_owned,) + block, jnp.float32),
            in_specs=[smem, smem, anywhere, anywhere, anywhere],
            out_specs=vmem,
            scratch_shapes=[
                pltpu.VMEM((4 * reach * bucket,) + block, jnp.float32),
                pltpu.VMEM(beside_shape.shape, jnp.float32),
                pltpu.VMEM((bucket,) + block, jnp.float32),
                pltpu.SMEM((4 * reach * bucket + 1,), jnp.int32),
                pltpu.SMEM((4 * reach * bucket + 1,), jnp.int32),
                pltpu.SemaphoreType.DMA((3,)),
            ],
            name="take",
        )(labels, table, send, recv.reshape((4 * reach * bucket,) + block), beside)
        return out.reshape(blocks_owned * cell_rows, flux)

    def padded(patches, pair_patch, pair_atm, numerators, counts, labels, table, send, recv, beside):
        return per_device(tiles, bands, patches, pair_patch, pair_atm, numerators, counts)

    overflowed = jnp.max(table[:, :, 0, LANES - 1]) > 0
    return lax.cond(overflowed, padded, take, patches, pair_patch, pair_atm, numerators, counts,
                    labels, table, send, recv, beside)


def solution(mesh):
    spec = P(("band", "tile"))
    placed = (
        P(("band", "tile"), None),
        spec,
        spec,
        P(("band", "tile"), None, None),
        spec,
    )
    body = functools.partial(adaptive, mesh.shape["tile"], mesh.shape["band"])
    return jax.shard_map(body, mesh=mesh, in_specs=placed, out_specs=P(("band", "tile"), None), check_vma=False)
```
